32 devices in a mesh: gx: 4 (over y, x), gy: 4 (over z), gz: 2 (over core).
Axes of the slice: x: 2, y: 2, z: 4, core: 2. Of those that a mesh axis runs over, the one named last changes fastest.
Arguments:
- grads: float32 [4, 4, 2, 160, 4096], P('gx', 'gy', 'gz'), may hold values from -6 to 6
- peer_table: int32 [4], replicated, may hold values from 0 to 3, each once
- layer_offsets: int32 [2], replicated, may hold values from 0 to 96, as said below
Outputs:
- averaged: float32 [4, 4, 2, 128, 4096], P('gx', 'gy', 'gz')
The draws below stay inside these ranges and needn't reach their ends.
Inputs may be any that keep to these rules, and one draw needn't show every extreme that they name: layer_offsets[l] is a multiple of 8 between l * (80) and l * 80 + 16; the last layer's offset is the largest of these.
All inputs are finite; a program needn't handle non-finite values.
Results may differ from the reference program's by a relative error of at most 0.00002.
Values sent between devices are 32-bit elements; how exact they have to be, the bound alone decides.
A program may use at most 64 MiB of HBM per device.

```python
import jax
import jax.numpy as jnp
from jax import lax

D = 4096
ROWS = 64
LAYERS = 2
SLACK = 16
BUF = 160
GB = 4
N_GX = 4
N_GY = 4
N_GZ = 2


def draw_layer_offsets(key, part):
    steps = jax.random.randint(key, (LAYERS,), 0, SLACK // 8 + 1)
    last = jnp.arange(LAYERS, dtype=jnp.int32) == LAYERS - 1
    steps = jnp.where(last, SLACK // 8, steps)
    starts = jnp.arange(LAYERS, dtype=jnp.int32) * (ROWS + SLACK)
    return (starts + 8 * steps).astype(jnp.int32)


def block_scale(rng, shape, shards, least, largest):
    level, own = 1.0, jax.random.fold_in(rng, 6)
    for axis_at, blocks in shards:
        draws = jnp.exp(jax.random.uniform(jax.random.fold_in(own, axis_at), (blocks,), jnp.float32, least / len(shards), largest / len(shards)))
        level = level * jnp.repeat(draws, shape[axis_at] // blocks).reshape([-1 if axis == axis_at else 1 for axis in range(len(shape))])
    return level


def scatter_about(key, extent, spread, most, cuts=(), kind=jnp.bfloat16):
    factor_of = block_scale(key, extent, cuts, -0.22, 0.18) if cuts else 1.0
    result = jax.random.normal(key, extent, jnp.float32) * spread * factor_of
    return jnp.minimum(jnp.maximum(result, -most), most).astype(kind)


def setup_inputs(seed: int = 0) -> dict:
    streams_of = jax.random.split(jax.random.key(seed), 4)
    return {
        "grads": scatter_about(streams_of[0], (N_GX, N_GY, N_GZ, BUF, D), 1.0, 6.0, ((0, 4), (1, 4), (2, 2)), jnp.float32),
        "peer_table": jax.random.permutation(streams_of[1], N_GY).astype(jnp.int32),
        "layer_offsets": draw_layer_offsets(jax.random.fold_in(streams_of[3], 71), 0),
    }


def reference(grads, peer_table, layer_offsets):
    pieces = [lax.dynamic_slice_in_dim(grads, layer_offsets[i].astype(jnp.int32), ROWS, 3) for i in range(LAYERS)]
    packed = jnp.concatenate(pieces, axis=3)
    logical = jnp.take(packed, peer_table, axis=1)
    shape = logical.shape
    mean_c = jnp.mean(logical, axis=2, keepdims=True)
    mixed = 0.5 * logical + 0.5 * mean_c
    upper = shape[1] // GB
    split = mixed.reshape(shape[0], upper, GB, shape[2], shape[3], shape[4])
    mean_b = jnp.mean(split, axis=2, keepdims=True)
    split = 0.5 * split + 0.5 * mean_b
    mean_a = jnp.mean(split, axis=(0, 1), keepdims=True)
    split = 0.5 * split + 0.5 * mean_a
    mixed = split.reshape(shape)
    averaged = jnp.zeros(shape, jnp.float32).at[:, peer_table].set(mixed)
    return averaged
```

```python
import functools

import jax
import jax.numpy as jnp
from jax import lax
from jax.experimental import pallas as pl
from jax.experimental.pallas import tpu as pltpu
from jax.sharding import PartitionSpec as P

ROWS = 64
LAYERS = 2
GROUP_B = 8
SUBLANES = 8
COLUMN_CUTS = 1
Z_LAG = 2
XY_LAG = 2
MESH = pl.DeviceIdType.MESH


def in_range(i, low, high):
    return jnp.logical_and(i >= low, i < high)


def mix_kernel(
    n, window, offsets, grads, out,
    win, mixed, value, up_in, up_out, down_in, down_out,
    half_in, part, part_in, full, full_in, core_out, core_in, result,
    load_sem, up_send, up_recv, down_send, down_recv,
    first_send, first_recv, second_send, second_recv, third_send, third_recv,
    core_send, core_recv, store_sem,
):
    chunks = value.shape[0]
    early = chunks // 2
    width = 2 * value.shape[3]
    cuts = out.shape[1] // width
    blocks = ROWS // SUBLANES

    square, z, core = lax.axis_index("gx"), lax.axis_index("gy"), lax.axis_index("gz")
    x, y = square % 2, square // 2
    across_x, across_y = y * 2 + (1 - x), (1 - y) * 2 + x
    first = across_x + core * (across_y - across_x)
    second = across_y + core * (across_x - across_y)
    mine = x + core * (y - x)
    other = 1 - mine
    has_lower, has_upper = z > 0, z < n - 1

    def load(layer):
        rows = pl.ds(layer * window, window)
        return pltpu.make_async_copy(grads.at[rows], win.at[layer], load_sem.at[layer])

    for layer in range(LAYERS):
        load(layer).start()

    barrier = pltpu.get_barrier_semaphore()
    for target in ({"gx": across_x}, {"gx": across_y}, {"gz": 1 - core}):
        pl.semaphore_signal(barrier, inc=1, device_id=target, device_id_type=MESH)

    @pl.when(has_lower)
    def _():
        pl.semaphore_signal(barrier, inc=1, device_id={"gy": z - 1}, device_id_type=MESH)

    @pl.when(has_upper)
    def _():
        pl.semaphore_signal(barrier, inc=1, device_id={"gy": z + 1}, device_id_type=MESH)

    def remote(src, dst, send, recv, i, target):
        return pltpu.make_async_remote_copy(
            src_ref=src, dst_ref=dst.at[i], send_sem=send.at[i], recv_sem=recv.at[i],
            device_id=target, device_id_type=MESH,
        )

    def up(i):
        return remote(up_out.at[i], up_in, up_send, up_recv, i, {"gy": z + 1})

    def down(i):
        return remote(down_out.at[i], down_in, down_send, down_recv, i, {"gy": z - 1})

    def halves(i):
        return remote(mixed.at[i, other], half_in, first_send, first_recv, i, {"gx": first})

    def parts(i):
        return remote(part.at[i], part_in, second_send, second_recv, i, {"gx": second})

    def fulls(i):
        return remote(full.at[i], full_in, third_send, third_recv, i, {"gx": first})

    def cores(i):
        return remote(core_out.at[i], core_in, core_send, core_recv, i, {"gz": 1 - core})

    def store(i, half):
        block, cut = i // cuts, i % cuts
        rows = pl.ds(pl.multiple_of(block * SUBLANES, SUBLANES), SUBLANES)
        columns = pl.ds(pl.multiple_of(cut * width + half * (width // 2), 128), width // 2)
        return pltpu.make_async_copy(result.at[i, half], out.at[rows, columns], store_sem.at[i, half])

    def unpack(layer, target):
        load(layer).wait()
        start = jnp.full((SUBLANES, width // 2), offsets[layer] - layer * window, jnp.int32)
        starts = range(0, window - ROWS + 1, SUBLANES)
        for block in range(blocks):
            top = block * SUBLANES
            for cut in range(cuts):
                i = (layer * blocks + block) * cuts + cut
                for half in range(2):
                    left = cut * width + half * (width // 2)
                    rows = win[layer, top:top + SUBLANES, left:left + width // 2]
                    for at in starts[1:]:
                        moved = win[layer, top + at:top + at + SUBLANES, left:left + width // 2]
                        rows = jnp.where(start == at, moved, rows)
                    target[i, half] = rows

    for layer in range(LAYERS):
        unpack(layer, value if layer < LAYERS // 2 else mixed)

    peers = 3 + jnp.where(has_lower, 1, 0) + jnp.where(has_upper, 1, 0)
    pl.semaphore_wait(barrier, peers)

    keep_z, keep_core, keep_x = 0.5 / n, 0.25, 0.125
    last = Z_LAG * (n - 1)

    def tick(t, carry):
        i = t - Z_LAG * z

        @pl.when(in_range(i, 0, chunks))
        def _():
            @pl.when(has_lower)
            def _():
                up(i).wait_recv()

            @pl.when(z == 0)
            def _():
                up_in[i] = jnp.zeros(up_in.shape[1:], up_in.dtype)

            @pl.when(has_upper)
            def _():
                up_out[i] = up_in[i] + value[i]
                up(i).start()

        j = t - Z_LAG * (n - 1 - z)

        @pl.when(in_range(j, 0, chunks))
        def _():
            @pl.when(has_upper)
            def _():
                down(j).wait_recv()

            @pl.when(z == n - 1)
            def _():
                down_in[j] = jnp.zeros(down_in.shape[1:], down_in.dtype)

            @pl.when(has_lower)
            def _():
                down_out[j] = down_in[j] + value[j]
                down(j).start()

        h = t

        @pl.when(in_range(h, 0, chunks - early))
        def _():
            halves(early + h).start()

        k = t - last

        @pl.when(in_range(k, 0, early))
        def _():
            core_out[k] = 0.5 * value[k] + keep_z * (value[k] + up_in[k] + down_in[k])
            cores(k).start()

        @pl.when(in_range(k, early, chunks))
        def _():
            result[k] = 0.5 * value[k] + keep_z * (value[k] + up_in[k] + down_in[k])
            for half in range(2):
                store(k, half).start()

        c = t - last - 1

        @pl.when(in_range(c, 0, early))
        def _():
            cores(c).wait_recv()
            mixed[c] = 0.75 * core_out[c] + keep_core * core_in[c]
            halves(c).start()

        def over_gx(i):
            @pl.when(in_range(i(0), *bounds))
            def _():
                s = i(0)
                halves(s).wait_recv()
                part[s] = mixed[s, mine] + half_in[s]
                parts(s).start()

            @pl.when(in_range(i(1), *bounds))
            def _():
                s = i(1)
                parts(s).wait_recv()
                full[s] = part[s] + part_in[s]
                fulls(s).start()

        bounds = (early, chunks)
        over_gx(lambda stage: early + t - XY_LAG * (stage + 1))
        late = early + t - 3 * XY_LAG

        @pl.when(in_range(late, early, chunks))
        def _():
            fulls(late).wait_recv()
            core_out[late, mine] = 0.5 * mixed[late, mine] + keep_x * full[late]
            core_out[late, other] = 0.5 * mixed[late, other] + keep_x * full_in[late]
            cores(late).start()

        swapped = late - 1

        @pl.when(in_range(swapped, early, chunks))
        def _():
            cores(swapped).wait_recv()
            value[swapped] = 0.75 * core_out[swapped] + keep_core * core_in[swapped]

        bounds = (0, early)
        over_gx(lambda stage: c - XY_LAG * (stage + 1))
        done = c - 3 * XY_LAG

        @pl.when(in_range(done, 0, early))
        def _():
            fulls(done).wait_recv()
            result[done, mine] = 0.5 * mixed[done, mine] + keep_x * full[done]
            result[done, other] = 0.5 * mixed[done, other] + keep_x * full_in[done]
            for half in range(2):
                store(done, half).start()

        return carry

    ticks = max(last + chunks, last + 1 + 3 * XY_LAG + early)
    lax.fori_loop(0, ticks, tick, 0)

    def drain(i, carry):
        @pl.when(has_upper)
        def _():
            up(i).wait_send()

        @pl.when(has_lower)
        def _():
            down(i).wait_send()

        halves(i).wait_send()
        parts(i).wait_send()
        fulls(i).wait_send()
        cores(i).wait_send()
        for half in range(2):
            store(i, half).wait()
        return carry

    lax.fori_loop(0, chunks, drain, 0)


def mix_in_kernel(grads, layer_offsets):
    buffer = grads[0, 0, 0]
    rows, columns = buffer.shape
    n = lax.axis_size("gy")
    window = rows // LAYERS
    chunks = LAYERS * ROWS // SUBLANES * COLUMN_CUTS
    half = columns // COLUMN_CUTS // 2
    whole = pltpu.VMEM((chunks, 2, SUBLANES, half), jnp.float32)
    piece = pltpu.VMEM((chunks, SUBLANES, half), jnp.float32)
    sems = pltpu.SemaphoreType.DMA((chunks,))
    result = pl.pallas_call(
        functools.partial(mix_kernel, n, window),
        out_shape=jax.ShapeDtypeStruct((LAYERS * ROWS, columns), jnp.float32),
        in_specs=[
            pl.BlockSpec(memory_space=pltpu.SMEM),
            pl.BlockSpec(memory_space=pl.ANY),
        ],
        out_specs=pl.BlockSpec(memory_space=pl.ANY),
        scratch_shapes=[
            pltpu.VMEM((LAYERS, window, columns), jnp.float32),
            whole, whole, whole, whole, whole, whole,
            piece, piece, piece, piece, piece, whole, whole, whole,
            pltpu.SemaphoreType.DMA((LAYERS,)),
            *([sems] * 12),
            pltpu.SemaphoreType.DMA((chunks, 2)),
        ],
        compiler_params=pltpu.CompilerParams(collective_id=0, has_side_effects=True),
    )(layer_offsets, buffer)
    return result[None, None, None]


def with_collectives(grads, peer_table, layer_offsets):
    buffer = grads[0, 0, 0]
    pieces = [lax.dynamic_slice_in_dim(buffer, layer_offsets[i], ROWS, 0) for i in range(LAYERS)]
    packed = jnp.concatenate(pieces, axis=0)
    count_y = lax.axis_size("gy")
    group_b = min(GROUP_B, count_y)
    group_a = lax.axis_size("gx") * (count_y // group_b)
    places = jnp.arange(count_y, dtype=jnp.int32)
    onehot = (peer_table[:, None] == places[None, :]).astype(jnp.int32)
    inverse = jnp.sum(onehot * places[:, None], axis=0)
    spread = lax.all_to_all(packed[None], "gy", split_axis=1, concat_axis=0, tiled=True)
    current = jnp.take(spread, peer_table, axis=0)
    total_c = lax.psum(current, "gz")
    current = 0.5 * current + 0.5 / lax.axis_size("gz") * total_c
    block_rows = current.shape[1]
    width = current.shape[2]
    split = current.reshape(count_y // group_b, group_b, block_rows, width)
    total_b = jnp.sum(split, axis=1, keepdims=True)
    split = 0.5 * split + 0.5 / group_b * total_b
    local_a = jnp.sum(split, axis=0, keepdims=True)
    total_a = lax.psum(local_a, "gx")
    split = 0.5 * split + 0.5 / group_a * total_a
    current = jnp.take(split.reshape(count_y, block_rows, width), inverse, axis=0)
    result = lax.all_to_all(current, "gy", split_axis=0, concat_axis=1, tiled=True)[0]
    return result[None, None, None]


def on_device(grads, peer_table, layer_offsets):
    one_group = lax.axis_size("gy") <= GROUP_B
    square_of_pairs = lax.axis_size("gx") == 4 and lax.axis_size("gz") == 2
    if one_group and square_of_pairs:
        return mix_in_kernel(grads, layer_offsets)
    return with_collectives(grads, peer_table, layer_offsets)


def solution(mesh):
    placed = (P("gx", "gy", "gz", None, None), P(), P())
    return jax.shard_map(
        on_device,
        mesh=mesh,
        in_specs=placed,
        out_specs=P("gx", "gy", "gz", None, None),
        check_vma=False,
    )
```

```python
import functools

import jax
import jax.numpy as jnp
from jax import lax
from jax.experimental import pallas as pl
from jax.experimental.pallas import tpu as pltpu
from jax.sharding import PartitionSpec as P

ROWS = 64
LAYERS = 2
GROUP_B = 8
SUBLANES = 8
COLUMN_CUTS = 2
Z_LAG = 3
Z_SLACK = 3
XY_LAG = 4
MIX_BYTES = 61 * 2**20
STORE_BYTES = 4 * 2**20
MESH = pl.DeviceIdType.MESH


def in_range(i, low, high):
    return jnp.logical_and(i >= low, i < high)


def mix_kernel(
    n, window, offsets, grads, result,
    win, mixed, value, up_in, up_out, down_in, down_out,
    half_in, part, part_in, full, full_in, core_out, core_in,
    load_sem, up_send, up_recv, down_send, down_recv,
    first_send, first_recv, second_send, second_recv, third_send, third_recv,
    core_send, core_recv,
):
    chunks = value.shape[0]
    early = chunks // 2
    width = 2 * value.shape[3]
    cuts = chunks * SUBLANES // (LAYERS * ROWS)
    blocks = ROWS // SUBLANES

    square, z, core = lax.axis_index("gx"), lax.axis_index("gy"), lax.axis_index("gz")
    x, y = square % 2, square // 2
    across_x, across_y = y * 2 + (1 - x), (1 - y) * 2 + x
    first = across_x + core * (across_y - across_x)
    second = across_y + core * (across_x - across_y)
    mine = x + core * (y - x)
    other = 1 - mine
    has_lower, has_upper = z > 0, z < n - 1

    def load(layer):
        rows = pl.ds(layer * window, window)
        return pltpu.make_async_copy(grads.at[rows], win.at[layer], load_sem.at[layer])

    for layer in range(LAYERS):
        load(layer).start()

    barrier = pltpu.get_barrier_semaphore()
    for target in ({"gx": across_x}, {"gx": across_y}, {"gz": 1 - core}):
        pl.semaphore_signal(barrier, inc=1, device_id=target, device_id_type=MESH)

    @pl.when(has_lower)
    def _():
        pl.semaphore_signal(barrier, inc=1, device_id={"gy": z - 1}, device_id_type=MESH)

    @pl.when(has_upper)
    def _():
        pl.semaphore_signal(barrier, inc=1, device_id={"gy": z + 1}, device_id_type=MESH)

    def remote(src, dst, send, recv, i, target):
        return pltpu.make_async_remote_copy(
            src_ref=src, dst_ref=dst.at[i], send_sem=send.at[0], recv_sem=recv.at[i],
            device_id=target, device_id_type=MESH,
        )

    def up(i):
        return remote(up_out.at[i], up_in, up_send, up_recv, i, {"gy": z + 1})

    def down(i):
        return remote(down_out.at[i], down_in, down_send, down_recv, i, {"gy": z - 1})

    def halves(i):
        return remote(mixed.at[i, other], half_in, first_send, first_recv, i, {"gx": first})

    def parts(i):
        return remote(part.at[i], part_in, second_send, second_recv, i, {"gx": second})

    def fulls(i):
        return remote(full.at[i], full_in, third_send, third_recv, i, {"gx": first})

    def cores(i):
        return remote(core_out.at[i], core_in, core_send, core_recv, i, {"gz": 1 - core})

    def unpack(layer, target):
        load(layer).wait()
        start = jnp.full((SUBLANES, width // 2), offsets[layer] - layer * window, jnp.int32)
        starts = range(0, window - ROWS + 1, SUBLANES)
        for block in range(blocks):
            top = block * SUBLANES
            for cut in range(cuts):
                i = (layer * blocks + block) * cuts + cut
                for half in range(2):
                    left = cut * width + half * (width // 2)
                    rows = win[layer, top:top + SUBLANES, left:left + width // 2]
                    for at in starts[1:]:
                        moved = win[layer, top + at:top + at + SUBLANES, left:left + width // 2]
                        rows = jnp.where(start == at, moved, rows)
                    target[i, half] = rows

    for layer in range(LAYERS // 2):
        unpack(layer, value)

    peers = 3 + jnp.where(has_lower, 1, 0) + jnp.where(has_upper, 1, 0)
    pl.semaphore_wait(barrier, peers)

    keep_z, keep_core, keep_x = 0.5 / n, 0.25, 0.125
    last = Z_LAG * (n - 1) + Z_SLACK

    def along_gy(t):
        def go_up():
            i = t - Z_LAG * z

            @pl.when(jnp.logical_and(has_upper, in_range(i, 0, chunks)))
            def _():
                @pl.when(has_lower)
                def _():
                    up(i).wait_recv()

                @pl.when(z == 0)
                def _():
                    up_in[i] = jnp.zeros(up_in.shape[1:], up_in.dtype)

                up_out[i] = up_in[i] + value[i]
                up(i).start()

        def go_down():
            j = t - Z_LAG * (n - 1 - z)

            @pl.when(jnp.logical_and(has_lower, in_range(j, 0, chunks)))
            def _():
                @pl.when(has_upper)
                def _():
                    down(j).wait_recv()

                @pl.when(z == n - 1)
                def _():
                    down_in[j] = jnp.zeros(down_in.shape[1:], down_in.dtype)

                down_out[j] = down_in[j] + value[j]
                down(j).start()

        far_above = z < n - 1 - z
        pl.when(far_above)(go_down)
        go_up()
        pl.when(jnp.logical_not(far_above))(go_down)

    def over_rest(t):
        h = t

        @pl.when(in_range(h, 0, chunks - early))
        def _():
            halves(early + h).start()

        k = t - last

        @pl.when(jnp.logical_and(z == 0, in_range(k, 0, chunks)))
        def _():
            down(k).wait_recv()

        @pl.when(jnp.logical_and(z == n - 1, in_range(k, 0, chunks)))
        def _():
            up(k).wait_recv()

        @pl.when(in_range(k, 0, early))
        def _():
            core_out[k] = 0.5 * value[k] + keep_z * (value[k] + up_in[k] + down_in[k])
            cores(k).start()

        @pl.when(in_range(k, early, chunks))
        def _():
            result[k] = 0.5 * value[k] + keep_z * (value[k] + up_in[k] + down_in[k])

        c = t - last - 1

        @pl.when(in_range(c, 0, early))
        def _():
            cores(c).wait_recv()
            mixed[c] = 0.75 * core_out[c] + keep_core * core_in[c]
            halves(c).start()

        def over_gx(i):
            @pl.when(in_range(i(0), *bounds))
            def _():
                s = i(0)
                halves(s).wait_recv()
                part[s] = mixed[s, mine] + half_in[s]
                parts(s).start()

            @pl.when(in_range(i(1), *bounds))
            def _():
                s = i(1)
                parts(s).wait_recv()
                full[s] = part[s] + part_in[s]
                fulls(s).start()

        bounds = (early, chunks)
        over_gx(lambda stage: early + t - XY_LAG * (stage + 1))
        late = early + t - 3 * XY_LAG

        @pl.when(in_range(late, early, chunks))
        def _():
            fulls(late).wait_recv()
            core_out[late, mine] = 0.5 * mixed[late, mine] + keep_x * full[late]
            core_out[late, other] = 0.5 * mixed[late, other] + keep_x * full_in[late]
            cores(late).start()

        swapped = late - 1

        @pl.when(in_range(swapped, early, chunks))
        def _():
            cores(swapped).wait_recv()
            value[swapped] = 0.75 * core_out[swapped] + keep_core * core_in[swapped]

        bounds = (0, early)
        over_gx(lambda stage: c - XY_LAG * (stage + 1))
        done = c - 3 * XY_LAG

        @pl.when(in_range(done, 0, early))
        def _():
            fulls(done).wait_recv()
            result[done, mine] = 0.5 * mixed[done, mine] + keep_x * full[done]
            result[done, other] = 0.5 * mixed[done, other] + keep_x * full_in[done]

    ticks = max(last + chunks, last + 1 + 3 * XY_LAG + early)
    along_gy(0)
    for layer in range(LAYERS // 2, LAYERS):
        unpack(layer, mixed)
    over_rest(0)

    def tick(t, carry):
        along_gy(t)
        over_rest(t)
        return carry

    lax.fori_loop(1, ticks, tick, 0)

    def sent(buffer, sem):
        pltpu.make_async_copy(buffer, buffer, sem.at[0]).wait()

    @pl.when(has_upper)
    def _():
        sent(up_out, up_send)

    @pl.when(has_lower)
    def _():
        sent(down_out, down_send)

    sent(half_in, first_send)
    sent(part, second_send)
    sent(full, third_send)
    sent(core_out, core_send)


def store_kernel(chunks, out, sem):
    count, _, _, half = chunks.shape
    cuts = count * SUBLANES // out.shape[0]
    copies = []
    for i in range(count):
        for side in range(2):
            top, left = i // cuts * SUBLANES, (i % cuts * 2 + side) * half
            target = out.at[top:top + SUBLANES, left:left + half]
            copies.append(pltpu.make_async_copy(chunks.at[i, side], target, sem.at[i, side]))
    for copy in copies:
        copy.start()
    for copy in copies:
        copy.wait()


def mix_in_kernel(grads, layer_offsets):
    buffer = grads[0, 0, 0]
    rows, columns = buffer.shape
    n = lax.axis_size("gy")
    window = rows // LAYERS
    chunks = LAYERS * ROWS // SUBLANES * COLUMN_CUTS
    half = columns // COLUMN_CUTS // 2
    whole = pltpu.VMEM((chunks, 2, SUBLANES, half), jnp.float32)
    piece = pltpu.VMEM((chunks, SUBLANES, half), jnp.float32)
    sems = pltpu.SemaphoreType.DMA((chunks,))
    mixed = pl.pallas_call(
        functools.partial(mix_kernel, n, window),
        out_shape=whole,
        in_specs=[
            pl.BlockSpec(memory_space=pltpu.SMEM),
            pl.BlockSpec(memory_space=pl.ANY),
        ],
        out_specs=pl.BlockSpec(memory_space=pltpu.VMEM),
        scratch_shapes=[
            pltpu.VMEM((LAYERS, window, columns), jnp.float32),
            whole, whole, whole, whole, whole, whole,
            piece, piece, piece, piece, piece, whole, whole,
            pltpu.SemaphoreType.DMA((LAYERS,)),
            *([pltpu.SemaphoreType.DMA((1,)), sems] * 6),
        ],
        compiler_params=pltpu.CompilerParams(
            collective_id=0, has_side_effects=True, vmem_limit_bytes=MIX_BYTES
        ),
    )(layer_offsets, buffer)
    result = pl.pallas_call(
        store_kernel,
        out_shape=jax.ShapeDtypeStruct((LAYERS * ROWS, columns), jnp.float32),
        in_specs=[pl.BlockSpec(memory_space=pltpu.VMEM)],
        out_specs=pl.BlockSpec(memory_space=pl.ANY),
        scratch_shapes=[pltpu.SemaphoreType.DMA((chunks, 2))],
        compiler_params=pltpu.CompilerParams(vmem_limit_bytes=STORE_BYTES),
    )(mixed)
    return result[None, None, None]


def with_collectives(grads, peer_table, layer_offsets):
    buffer = grads[0, 0, 0]
    pieces = [lax.dynamic_slice_in_dim(buffer, layer_offsets[i], ROWS, 0) for i in range(LAYERS)]
    packed = jnp.concatenate(pieces, axis=0)
    count_y = lax.axis_size("gy")
    group_b = min(GROUP_B, count_y)
    group_a = lax.axis_size("gx") * (count_y // group_b)
    places = jnp.arange(count_y, dtype=jnp.int32)
    onehot = (peer_table[:, None] == places[None, :]).astype(jnp.int32)
    inverse = jnp.sum(onehot * places[:, None], axis=0)
    spread = lax.all_to_all(packed[None], "gy", split_axis=1, concat_axis=0, tiled=True)
    current = jnp.take(spread, peer_table, axis=0)
    total_c = lax.psum(current, "gz")
    current = 0.5 * current + 0.5 / lax.axis_size("gz") * total_c
    block_rows = current.shape[1]
    width = current.shape[2]
    split = current.reshape(count_y // group_b, group_b, block_rows, width)
    total_b = jnp.sum(split, axis=1, keepdims=True)
    split = 0.5 * split + 0.5 / group_b * total_b
    local_a = jnp.sum(split, axis=0, keepdims=True)
    total_a = lax.psum(local_a, "gx")
    split = 0.5 * split + 0.5 / group_a * total_a
    current = jnp.take(split.reshape(count_y, block_rows, width), inverse, axis=0)
    result = lax.all_to_all(current, "gy", split_axis=0, concat_axis=1, tiled=True)[0]
    return result[None, None, None]


def on_device(grads, peer_table, layer_offsets):
    one_group = lax.axis_size("gy") <= GROUP_B
    square_of_pairs = lax.axis_size("gx") == 4 and lax.axis_size("gz") == 2
    if one_group and square_of_pairs and lax.axis_size("gy") > 1:
        return mix_in_kernel(grads, layer_offsets)
    return with_collectives(grads, peer_table, layer_offsets)


def solution(mesh):
    placed = (P("gx", "gy", "gz", None, None), P(), P())
    return jax.shard_map(
        on_device,
        mesh=mesh,
        in_specs=placed,
        out_specs=P("gx", "gy", "gz", None, None),
        check_vma=False,
    )
```

```python
import functools

import jax
import jax.numpy as jnp
from jax import lax
from jax.experimental import pallas as pl
from jax.experimental.pallas import tpu as pltpu
from jax.sharding import PartitionSpec as P

ROWS = 64
LAYERS = 2
GROUP_B = 8
SUBLANES = 8
COLUMN_CUTS = 2
Z_LAG = 3
Z_SLACK = 3
XY_LAG = 4
MIX_BYTES = 61 * 2**20
STORE_BYTES = 4 * 2**20
MESH = pl.DeviceIdType.MESH


def in_range(i, low, high):
    return jnp.logical_and(i >= low, i < high)


def mix_kernel(
    n, window, offsets, grads, result,
    win, mixed, value, up_in, up_out, down_in, down_out,
    half_in, part, part_in, full, full_in, core_out, core_in,
    load_sem, up_send, up_recv, down_send, down_recv,
    first_send, first_recv, second_send, second_recv, third_send, third_recv,
    core_send, core_recv,
):
    chunks = value.shape[0]
    early = chunks // 2
    width = 2 * value.shape[3]
    cuts = chunks * SUBLANES // (LAYERS * ROWS)
    blocks = ROWS // SUBLANES

    square, z, core = lax.axis_index("gx"), lax.axis_index("gy"), lax.axis_index("gz")
    x, y = square % 2, square // 2
    across_x, across_y = y * 2 + (1 - x), (1 - y) * 2 + x
    first = across_x + core * (across_y - across_x)
    second = across_y + core * (across_x - across_y)
    mine = x + core * (y - x)
    other = 1 - mine
    has_lower, has_upper = z > 0, z < n - 1

    def load(layer):
        rows = pl.ds(layer * window, window)
        return pltpu.make_async_copy(grads.at[rows], win.at[layer], load_sem.at[layer])

    for layer in range(LAYERS // 2):
        load(layer).start()

    barrier = pltpu.get_barrier_semaphore()
    for target in ({"gx": across_x}, {"gx": across_y}, {"gz": 1 - core}):
        pl.semaphore_signal(barrier, inc=1, device_id=target, device_id_type=MESH)

    @pl.when(has_lower)
    def _():
        pl.semaphore_signal(barrier, inc=1, device_id={"gy": z - 1}, device_id_type=MESH)

    @pl.when(has_upper)
    def _():
        pl.semaphore_signal(barrier, inc=1, device_id={"gy": z + 1}, device_id_type=MESH)

    def remote(src, dst, send, recv, i, target):
        return pltpu.make_async_remote_copy(
            src_ref=src, dst_ref=dst.at[i], send_sem=send.at[0], recv_sem=recv.at[i],
            device_id=target, device_id_type=MESH,
        )

    def up(i):
        return remote(up_out.at[i], up_in, up_send, up_recv, i, {"gy": z + 1})

    def down(i):
        return remote(down_out.at[i], down_in, down_send, down_recv, i, {"gy": z - 1})

    def halves(i):
        return remote(mixed.at[i, other], half_in, first_send, first_recv, i, {"gx": first})

    def parts(i):
        return remote(part.at[i], part_in, second_send, second_recv, i, {"gx": second})

    def fulls(i):
        return remote(full.at[i], full_in, third_send, third_recv, i, {"gx": first})

    def cores(i):
        return remote(core_out.at[i], core_in, core_send, core_recv, i, {"gz": 1 - core})

    def unpack(layer, target):
        load(layer).wait()
        start = jnp.full((SUBLANES, width // 2), offsets[layer] - layer * window, jnp.int32)
        starts = range(0, window - ROWS + 1, SUBLANES)
        for block in range(blocks):
            top = block * SUBLANES
            for cut in range(cuts):
                i = (layer * blocks + block) * cuts + cut
                for half in range(2):
                    left = cut * width + half * (width // 2)
                    rows = win[layer, top:top + SUBLANES, left:left + width // 2]
                    for at in starts[1:]:
                        moved = win[layer, top + at:top + at + SUBLANES, left:left + width // 2]
                        rows = jnp.where(start == at, moved, rows)
                    target[i, half] = rows

    for layer in range(LAYERS // 2):
        unpack(layer, value)
    for layer in range(LAYERS // 2, LAYERS):
        load(layer).start()

    peers = 3 + jnp.where(has_lower, 1, 0) + jnp.where(has_upper, 1, 0)
    pl.semaphore_wait(barrier, peers)

    keep_z, keep_core, keep_x = 0.5 / n, 0.25, 0.125
    last = Z_LAG * (n - 1) + Z_SLACK

    def along_gy(t):
        def go_up():
            i = t - Z_LAG * z

            @pl.when(jnp.logical_and(has_upper, in_range(i, 0, chunks)))
            def _():
                @pl.when(has_lower)
                def _():
                    up(i).wait_recv()

                @pl.when(z == 0)
                def _():
                    up_in[i] = jnp.zeros(up_in.shape[1:], up_in.dtype)

                up_out[i] = up_in[i] + value[i]
                up(i).start()

        def go_down():
            j = t - Z_LAG * (n - 1 - z)

            @pl.when(jnp.logical_and(has_lower, in_range(j, 0, chunks)))
            def _():
                @pl.when(has_upper)
                def _():
                    down(j).wait_recv()

                @pl.when(z == n - 1)
                def _():
                    down_in[j] = jnp.zeros(down_in.shape[1:], down_in.dtype)

                down_out[j] = down_in[j] + value[j]
                down(j).start()

        far_above = z < n - 1 - z
        pl.when(far_above)(go_down)
        go_up()
        pl.when(jnp.logical_not(far_above))(go_down)

    def over_rest(t):
        h = t

        @pl.when(in_range(h, 0, chunks - early))
        def _():
            halves(early + h).start()

        k = t - last

        @pl.when(jnp.logical_and(z == 0, in_range(k, 0, chunks)))
        def _():
            down(k).wait_recv()

        @pl.when(jnp.logical_and(z == n - 1, in_range(k, 0, chunks)))
        def _():
            up(k).wait_recv()

        @pl.when(in_range(k, 0, early))
        def _():
            core_out[k] = 0.5 * value[k] + keep_z * (value[k] + up_in[k] + down_in[k])
            cores(k).start()

        @pl.when(in_range(k, early, chunks))
        def _():
            result[k] = 0.5 * value[k] + keep_z * (value[k] + up_in[k] + down_in[k])

        c = t - last - 1

        @pl.when(in_range(c, 0, early))
        def _():
            cores(c).wait_recv()
            mixed[c] = 0.75 * core_out[c] + keep_core * core_in[c]
            halves(c).start()

        def over_gx(i):
            @pl.when(in_range(i(0), *bounds))
            def _():
                s = i(0)
                halves(s).wait_recv()
                part[s] = mixed[s, mine] + half_in[s]
                parts(s).start()

            @pl.when(in_range(i(1), *bounds))
            def _():
                s = i(1)
                parts(s).wait_recv()
                full[s] = part[s] + part_in[s]
                fulls(s).start()

        bounds = (early, chunks)
        over_gx(lambda stage: early + t - XY_LAG * (stage + 1))
        late = early + t - 3 * XY_LAG

        @pl.when(in_range(late, early, chunks))
        def _():
            fulls(late).wait_recv()
            core_out[late, mine] = 0.5 * mixed[late, mine] + keep_x * full[late]
            core_out[late, other] = 0.5 * mixed[late, other] + keep_x * full_in[late]
            cores(late).start()

        swapped = late - 1

        @pl.when(in_range(swapped, early, chunks))
        def _():
            cores(swapped).wait_recv()
            value[swapped] = 0.75 * core_out[swapped] + keep_core * core_in[swapped]

        bounds = (0, early)
        over_gx(lambda stage: c - XY_LAG * (stage + 1))
        done = c - 3 * XY_LAG

        @pl.when(in_range(done, 0, early))
        def _():
            fulls(done).wait_recv()
            result[done, mine] = 0.5 * mixed[done, mine] + keep_x * full[done]
            result[done, other] = 0.5 * mixed[done, other] + keep_x * full_in[done]

    ticks = max(last + chunks, last + 1 + 3 * XY_LAG + early)
    along_gy(0)
    for layer in range(LAYERS // 2, LAYERS):
        unpack(layer, mixed)
    over_rest(0)

    def tick(t, carry):
        along_gy(t)
        over_rest(t)
        return carry

    lax.fori_loop(1, ticks, tick, 0)

    def sent(buffer, sem):
        pltpu.make_async_copy(buffer, buffer, sem.at[0]).wait()

    @pl.when(has_upper)
    def _():
        sent(up_out, up_send)

    @pl.when(has_lower)
    def _():
        sent(down_out, down_send)

    sent(half_in, first_send)
    sent(part, second_send)
    sent(full, third_send)
    sent(core_out, core_send)


def store_kernel(chunks, out, sem):
    count, _, _, half = chunks.shape
    cuts = count * SUBLANES // out.shape[0]
    copies = []
    for i in range(count):
        for side in range(2):
            top, left = i // cuts * SUBLANES, (i % cuts * 2 + side) * half
            target = out.at[top:top + SUBLANES, left:left + half]
            copies.append(pltpu.make_async_copy(chunks.at[i, side], target, sem.at[i, side]))
    for copy in copies:
        copy.start()
    for copy in copies:
        copy.wait()


def mix_in_kernel(grads, layer_offsets):
    buffer = grads[0, 0, 0]
    rows, columns = buffer.shape
    n = lax.axis_size("gy")
    window = rows // LAYERS
    chunks = LAYERS * ROWS // SUBLANES * COLUMN_CUTS
    half = columns // COLUMN_CUTS // 2
    whole = pltpu.VMEM((chunks, 2, SUBLANES, half), jnp.float32)
    piece = pltpu.VMEM((chunks, SUBLANES, half), jnp.float32)
    sems = pltpu.SemaphoreType.DMA((chunks,))
    mixed = pl.pallas_call(
        functools.partial(mix_kernel, n, window),
        out_shape=whole,
        in_specs=[
            pl.BlockSpec(memory_space=pltpu.SMEM),
            pl.BlockSpec(memory_space=pl.ANY),
        ],
        out_specs=pl.BlockSpec(memory_space=pltpu.VMEM),
        scratch_shapes=[
            pltpu.VMEM((LAYERS, window, columns), jnp.float32),
            whole, whole, whole, whole, whole, whole,
            piece, piece, piece, piece, piece, whole, whole,
            pltpu.SemaphoreType.DMA((LAYERS,)),
            *([pltpu.SemaphoreType.DMA((1,)), sems] * 6),
        ],
        compiler_params=pltpu.CompilerParams(
            collective_id=0, has_side_effects=True, vmem_limit_bytes=MIX_BYTES
        ),
    )(layer_offsets, buffer)
    result = pl.pallas_call(
        store_kernel,
        out_shape=jax.ShapeDtypeStruct((LAYERS * ROWS, columns), jnp.float32),
        in_specs=[pl.BlockSpec(memory_space=pltpu.VMEM)],
        out_specs=pl.BlockSpec(memory_space=pl.ANY),
        scratch_shapes=[pltpu.SemaphoreType.DMA((chunks, 2))],
        compiler_params=pltpu.CompilerParams(vmem_limit_bytes=STORE_BYTES),
    )(mixed)
    return result[None, None, None]


def with_collectives(grads, peer_table, layer_offsets):
    buffer = grads[0, 0, 0]
    pieces = [lax.dynamic_slice_in_dim(buffer, layer_offsets[i], ROWS, 0) for i in range(LAYERS)]
    packed = jnp.concatenate(pieces, axis=0)
    count_y = lax.axis_size("gy")
    group_b = min(GROUP_B, count_y)
    group_a = lax.axis_size("gx") * (count_y // group_b)
    places = jnp.arange(count_y, dtype=jnp.int32)
    onehot = (peer_table[:, None] == places[None, :]).astype(jnp.int32)
    inverse = jnp.sum(onehot * places[:, None], axis=0)
    spread = lax.all_to_all(packed[None], "gy", split_axis=1, concat_axis=0, tiled=True)
    current = jnp.take(spread, peer_table, axis=0)
    total_c = lax.psum(current, "gz")
    current = 0.5 * current + 0.5 / lax.axis_size("gz") * total_c
    block_rows = current.shape[1]
    width = current.shape[2]
    split = current.reshape(count_y // group_b, group_b, block_rows, width)
    total_b = jnp.sum(split, axis=1, keepdims=True)
    split = 0.5 * split + 0.5 / group_b * total_b
    local_a = jnp.sum(split, axis=0, keepdims=True)
    total_a = lax.psum(local_a, "gx")
    split = 0.5 * split + 0.5 / group_a * total_a
    current = jnp.take(split.reshape(count_y, block_rows, width), inverse, axis=0)
    result = lax.all_to_all(current, "gy", split_axis=0, concat_axis=1, tiled=True)[0]
    return result[None, None, None]


def on_device(grads, peer_table, layer_offsets):
    one_group = lax.axis_size("gy") <= GROUP_B
    square_of_pairs = lax.axis_size("gx") == 4 and lax.axis_size("gz") == 2
    if one_group and square_of_pairs and lax.axis_size("gy") > 1:
        return mix_in_kernel(grads, layer_offsets)
    return with_collectives(grads, peer_table, layer_offsets)


def solution(mesh):
    placed = (P("gx", "gy", "gz", None, None), P(), P())
    return jax.shard_map(
        on_device,
        mesh=mesh,
        in_specs=placed,
        out_specs=P("gx", "gy", "gz", None, None),
        check_vma=False,
    )
```
